32 devices in a mesh: ta: 4 (over y, x), row: 4 (over z), col: 2 (over core).
Axes of the slice: x: 2, y: 2, z: 4, core: 2. Of those that a mesh axis runs over, the one named last changes fastest.
Arguments:
- latent_in: float32 [64, 64, 48, 384], P('ta', 'row', 'col'), may hold values from -6 to 6
- norm_gains: float32 [2, 384], replicated, may hold values from 0.1 to 1.9
- conv_weights: bfloat16 [2, 3, 3, 3, 384, 384], replicated, may hold values from -0.0625 to 0.0625
- conv_bias: float32 [2, 384], replicated, may hold values from -3 to 3
Outputs:
- latent_out: float32 [64, 64, 48, 384], P('ta', 'row', 'col')
The draws below stay inside these ranges and needn't reach their ends.
All inputs are finite; a program needn't handle non-finite values.
Results may differ from the reference program's by a relative error of at most 0.002.
Values may be sent and summed in bfloat16 or wider, within the bound.
No kernel may reach another device: no remote copies, remote signals or barrier semaphores. Data moves between devices by JAX's collectives and lax.ppermute only.
A program may use at most 192 MiB of HBM per device.

```python
import jax
import jax.numpy as jnp
from jax import lax

C = 384
H = 64
W = 48
FRAMES = 64


def block_scale(key, extent, pieces, smallest, largest):
    loudness, own = 1.0, jax.random.fold_in(key, 6)
    for axis_at, blocks in pieces:
        heights = jnp.exp(jax.random.uniform(jax.random.fold_in(own, axis_at), (blocks,), jnp.float32, smallest / len(pieces), largest / len(pieces)))
        loudness = loudness * jnp.repeat(heights, extent[axis_at] // blocks).reshape([-1 if axis == axis_at else 1 for axis in range(len(extent))])
    return loudness


def noise(own_key, extent, deviation, bound, pieces=(), held_as=jnp.bfloat16):
    values = deviation * jax.random.normal(own_key, extent, jnp.float32)
    if pieces:
        values = values * block_scale(own_key, extent, pieces, -0.22, 0.18)
    return jnp.clip(values, -bound, bound).astype(held_as)


def setup_inputs(seed: int = 0) -> dict:
    key_list = jax.random.split(jax.random.key(seed), 5)
    return {
        "latent_in": noise(key_list[0], (FRAMES, H, W, C), 1.0, 6.0, ((0, 4), (1, 4), (2, 2)), jnp.float32),
        "norm_gains": jnp.clip(1.0 + 0.18 * jax.random.normal(key_list[1], (2, C), jnp.float32), 0.1, 1.9),
        "conv_weights": noise(key_list[2], (2, 3, 3, 3, C, C), (27 * C) ** -0.5, 0.0625),
        "conv_bias": noise(key_list[3], (2, C), 0.5, 3.0, (), jnp.float32),
    }


EPS = 1e-06

def activate(value, gain):
    mean_sq = lax.optimization_barrier(jnp.mean(value * value, axis=-1, keepdims=True))
    return jax.nn.silu(value * lax.rsqrt(mean_sq + EPS) * gain).astype(jnp.bfloat16)

def causal_conv(acts, weight, bias):
    padded = jnp.pad(acts, ((2, 0), (1, 1), (1, 1), (0, 0)))
    height = acts.shape[1]
    width = acts.shape[2]
    chans = acts.shape[3]

    def one_frame(frame):
        window = lax.dynamic_slice_in_dim(padded, frame, 3, 0)
        total = jnp.zeros((height * width, weight.shape[-1]), jnp.float32)
        for tap_t in range(3):
            for tap_r in range(3):
                for tap_c in range(3):
                    piece = window[tap_t, tap_r:tap_r + height, tap_c:tap_c + width].reshape(-1, chans)
                    total = total + jnp.dot(piece, weight[tap_t, tap_r, tap_c], preferred_element_type=jnp.float32)
        return (total + bias).reshape(height, width, -1)
    return lax.map(one_frame, jnp.arange(acts.shape[0], dtype=jnp.int32))

def reference(latent_in, norm_gains, conv_weights, conv_bias):
    first = causal_conv(activate(latent_in, norm_gains[0]), conv_weights[0], conv_bias[0])
    second = causal_conv(activate(first, norm_gains[1]), conv_weights[1], conv_bias[1])
    return latent_in + second
```

```python
import jax
import jax.numpy as jnp
from jax import lax
from jax.experimental import pallas as pl
from jax.experimental.pallas import tpu as pltpu
from jax.sharding import PartitionSpec as P

EPS = 1e-06
PARITY = True
SUB = 8
LANE = 128
F32 = jnp.float32
BF16 = jnp.bfloat16


def activate(value, gain):
    mean_sq = jnp.mean(value * value, axis=-1, keepdims=True)
    u = value * lax.rsqrt(mean_sq + EPS) * gain
    return (u / (1.0 + jnp.exp(-u))).astype(BF16)


def border_parts(value, r, j, half, blocks, last_valid):
    parts = []
    if r == 0:
        parts.append(("row", 0, j * SUB, value[0:SUB]))
    if r == half - 1:
        parts.append(("row", 1, j * SUB, value[SUB:16]))
    if j == 0:
        parts.append(("col", 0, r, value[0:1]))
        parts.append(("col", 0, r + half, value[SUB : SUB + 1]))
    if j == blocks - 1:
        parts.append(("col", 1, r, value[last_valid : last_valid + 1]))
        parts.append(("col", 1, r + half, value[SUB + last_valid : SUB + last_valid + 1]))
    return parts


def prepare_kernel(last_valid, x_ref, gain_ref, out_ref, row0, row1, col0, col1, tail_ref, row_f, col_f):
    half, blocks = x_ref.shape[1] // 2, x_ref.shape[2] // SUB
    gain = gain_ref[...]
    for r in range(half):
        for j in range(blocks):
            cols = pl.ds(j * SUB, SUB)
            v = jnp.concatenate([x_ref[0, r, cols, :], x_ref[0, r + half, cols, :]], axis=0)
            a = activate(v, gain)
            out_ref[0, pl.ds((r * blocks + j) * 16, 16), :] = a
            tail_ref[0, pl.ds((r * blocks + j) * 16, 16), :] = a
            for kind, e, row, piece in border_parts(a.astype(F32), r, j, half, blocks, last_valid):
                dst = row_f if kind == "row" else col_f
                dst[e, pl.ds(row, piece.shape[0]), :] = piece
    row0[0] = row_f[0].astype(BF16)
    row1[0] = row_f[1].astype(BF16)
    col0[0] = col_f[0].astype(BF16)
    col1[0] = col_f[1].astype(BF16)


def prepare(x, gain, width):
    frames, rows, cols, chans = x.shape
    cells = rows * cols

    def spec(n):
        return pl.BlockSpec((1, n, chans), lambda f: (f, 0, 0))

    sizes = (cells, cols, cols, rows, rows)
    return pl.pallas_call(
        lambda *refs: prepare_kernel((width - 1) % SUB, *refs),
        out_shape=[jax.ShapeDtypeStruct((frames, n, chans), BF16) for n in sizes]
        + [jax.ShapeDtypeStruct((2, cells, chans), BF16)],
        grid=(frames,),
        in_specs=[
            pl.BlockSpec((1, rows, cols, chans), lambda f: (f, 0, 0, 0)),
            pl.BlockSpec((1, chans), lambda f: (0, 0)),
        ],
        out_specs=[spec(n) for n in sizes]
        + [pl.BlockSpec((1, cells, chans), lambda f: (jnp.maximum(f - (frames - 2), 0), 0, 0))],
        scratch_shapes=[pltpu.VMEM((2, cols, chans), F32), pltpu.VMEM((2, rows, chans), F32)],
        compiler_params=pltpu.CompilerParams(vmem_limit_bytes=60 << 20),
        cost_estimate=pl.CostEstimate(flops=20 * x.size, bytes_accessed=6 * x.size, transcendentals=2 * x.size),
        name="prepare",
    )(x, gain)


def conv_kernel(cfg, *refs):
    segs, n_ops, n_in, rows, blocks, chans, layer, last_valid, final, x_start = cfg
    n_out = n_in - 2
    steps = n_out // 2
    half = rows // 2
    cols = blocks * SUB
    wide = blocks * 16
    n_chunk = chans // LANE
    ins = refs[:n_ops]
    at = n_ops
    flag_ref, parity_ref, w_hbm, bias_ref, gain_ref = refs[at : at + 5]
    at += 5
    if final:
        x_hbm = refs[at]
        at += 2 if final == 2 else 1
        outs = refs[at : at + 1]
        at += 1
    else:
        outs = refs[at : at + 6]
        at += 6
    (a_buf, w_buf, t_buf, edge_buf, side_buf, corner_buf, edge_f, side_f, corner_f, pm, p3, o_buf,
     row_f, col_f, row_buf, col_buf, in_sem, w_sem, x_sem, o_sem, b_sem) = refs[at:]
    taps = [(dt, dr, dc) for dt in range(3) for dr in range(3) for dc in range(3)]
    slots = (parity_ref[0], 1 - parity_ref[0])

    copies = []

    def fetch(src, dst):
        copies.append(pltpu.make_async_copy(src, dst, in_sem.at[len(copies)]))

    base = 0
    corner_at = 0
    corners = []
    for kind, which, start, count in segs:
        here = pl.ds(base, count)
        if kind == "own":
            t, top, bot, lft, rgt = [ins[n] for n in which]
            there = pl.ds(start, count)
            fetch(t.at[there], t_buf.at[here])
            frames = t.shape[0]
            extra = top.shape[0] - frames
            for e, part in ((0, top), (1, bot)):
                fetch(part.at[there], edge_buf.at[e, here])
                fetch(part.at[pl.ds(frames, extra)], corner_buf.at[e, pl.ds(corner_at, extra)])
                corners.append((e, e, corner_at, extra, 2 * start, base, count))
            for e, part in ((0, lft), (1, rgt)):
                fetch(part.at[there], side_buf.at[e, here])
            corner_at += extra
        else:
            t, rec = [ins[n] for n in which]
            fetch(t, t_buf.at[here])
            for e in range(2):
                fetch(rec.at[:, pl.ds(e * cols, cols)], edge_buf.at[e, here])
                fetch(rec.at[:, pl.ds(2 * cols + e * rows, rows)], side_buf.at[e, here])
            fetch(rec.at[:, pl.ds(2 * (cols + rows), SUB)], corner_buf.at[0, pl.ds(corner_at, count), pl.ds(0, SUB)])
            for e in range(2):
                for k in range(count):
                    corners.append((e, 0, corner_at + k, 1, 2 * e, base + k, 1))
            corner_at += count
        base += count
    w_copies = [
        pltpu.make_async_copy(
            w_hbm.at[layer, dt, :, :, :, pl.ds(oc * LANE, LANE)], w_buf.at[oc, dt], w_sem.at[dt, oc]
        )
        for dt in range(3)
        for oc in range(n_chunk)
    ]
    for c in copies:
        c.start()
    for c in w_copies:
        c.start()
    if final:
        x_copy = pltpu.make_async_copy(x_hbm.at[pl.ds(x_start, n_out)], o_buf, x_sem)
        x_copy.start()
    for c in copies:
        c.wait()

    def widen(f, carry):
        for e in range(2):
            edge_f[e, f] = edge_buf[e, f].astype(F32)
            side_f[e, f] = side_buf[e, f].astype(F32) * flag_ref[e]
        return carry

    lax.fori_loop(0, n_in, widen, 0)
    for e, source, where, extra, first, base_, count in corners:
        block = corner_buf[source, pl.ds(where, extra)].astype(F32).reshape(extra * cols, chans)
        corner_f[e, pl.ds(2 * base_, 2 * count), :] = block[first : first + 2 * count]

    sub_index = lax.broadcasted_iota(jnp.int32, (SUB, chans), 0)
    is_first = sub_index == 0
    is_last = sub_index == SUB - 1
    is_valid_last = sub_index == last_valid

    def tile_at(f, r, j):
        return t_buf[f, pl.ds((r * blocks + j) * 16, 16), :]

    def beside(e, f, row):
        if row < 0 or row >= rows:
            value = corner_f[slots[0 if row < 0 else 1], pl.ds(2 * f + e, 1), :] * flag_ref[e]
        else:
            value = side_f[e, f, pl.ds(row, 1), :]
        return jnp.broadcast_to(value, (SUB, chans))

    def build(f, rs):
        tiles = []
        for j in range(blocks):
            if 1 <= rs <= half:
                tiles.append(tile_at(f, rs - 1, j))
            elif rs == 0:
                upper = edge_f[slots[0], f, pl.ds(j * SUB, SUB), :]
                lower = tile_at(f, half - 1, j).astype(F32)[0:SUB]
                tiles.append(jnp.concatenate([upper, lower], axis=0).astype(BF16))
            else:
                upper = tile_at(f, 0, j).astype(F32)[SUB:16]
                lower = edge_f[slots[1], f, pl.ds(j * SUB, SUB), :]
                tiles.append(jnp.concatenate([upper, lower], axis=0).astype(BF16))
        shifted = [[[None, None] for _ in range(blocks)] for _ in range(2)]
        for h in range(2):
            row = rs - 1 + half * h
            left = beside(0, f, row)
            right = beside(1, f, row)
            parts = [t.astype(F32)[h * SUB : (h + 1) * SUB] for t in tiles]
            down = [left] + [pltpu.roll(p, 1, 0) for p in parts]
            up = [pltpu.roll(p, SUB - 1, 0) for p in parts]
            for j in range(blocks):
                shifted[0][j][h] = jnp.where(is_first, down[j], down[j + 1])
                if j + 1 < blocks:
                    shifted[1][j][h] = jnp.where(is_last, up[j + 1], up[j])
                else:
                    shifted[1][j][h] = jnp.where(is_valid_last, right, up[j])
        stores = []
        for j in range(blocks):
            low = jnp.concatenate(shifted[0][j], axis=0).astype(BF16)
            high = jnp.concatenate(shifted[1][j], axis=0).astype(BF16)
            for dc, value in ((0, low), (1, tiles[j]), (2, high)):
                for kc in range(n_chunk):
                    part = value[:, kc * LANE : (kc + 1) * LANE]
                    stores.append((a_buf, (kc, dc, f, rs, pl.ds(j * 16, 16), slice(None)), part))
        return stores

    def put(stores):
        for ref, index, value in stores:
            ref[index] = value

    def finish(q, f, r, j, live=None):
        if r == half:
            stores = []
            for e in range(2):
                stores.append((row_buf, (e, f), row_f[q, e].astype(BF16)))
                stores.append((col_buf, (e, f), col_f[q, e].astype(BF16)))
            return stores
        sl = pl.ds(j * 16, 16)
        v = jnp.concatenate([pm[q, r, sl, :], p3[q, r, sl, :]], axis=1) + bias_ref[...]
        if not final:
            a = activate(v, gain_ref[...])
            stores = [(o_buf, (f, pl.ds((r * blocks + j) * 16, 16), slice(None)), a)]
            for kind, e, row, piece in border_parts(a.astype(F32), r, j, half, blocks, last_valid):
                dst = row_f if kind == "row" else col_f
                stores.append((dst, (q, e, pl.ds(row, piece.shape[0]), slice(None)), piece))
            return stores
        stores = []
        for h in range(2):
            index = (f, r + half * h, pl.ds(j * SUB, SUB), slice(None))
            part = v[h * SUB : (h + 1) * SUB]
            if live is not None:
                part = jnp.where(live, part, 0.0)
            stores.append((o_buf, index, o_buf[index] + part))
        return stores

    units = [(r, j) for r in range(half) for j in range(blocks)]
    if not final:
        units.append((half, 0))

    main_chunks = [(tap, kc) for tap in taps for kc in range(n_chunk)]
    pair_chunks = [
        ((dt, drp, dc), kc)
        for dt in range(3) for drp in range(4) for dc in range(3) for kc in range(n_chunk)
    ]

    def main_weight(chunk):
        if chunk is None:
            return jnp.zeros((LANE, 2 * LANE), BF16)
        (dt, dr, dc), kc = chunk
        here = pl.ds(kc * LANE, LANE)
        return jnp.concatenate([w_buf[0, dt, dr, dc, here, :], w_buf[1, dt, dr, dc, here, :]], axis=1)

    def pair_weight(chunk):
        (dt, drp, dc), kc = chunk
        sides = []
        for dr in (drp, drp - 1):
            if 0 <= dr <= 2:
                sides.append(w_buf[2, dt, dr, dc, pl.ds(kc * LANE, LANE), :])
            else:
                sides.append(jnp.zeros((LANE, LANE), BF16))
        return jnp.concatenate(sides, axis=1)

    def lhs_piece(chunk, o, r):
        (dt, dr, dc), kc = chunk
        return a_buf[kc, dc, o + dt, r + dr]

    def run_pass(chunks, k, weight, accs, o, row_of):
        one = chunks[2 * k]
        two = chunks[2 * k + 1] if 2 * k + 1 < len(chunks) else None
        w = jnp.concatenate([weight(one), weight(two)], axis=0)
        reg = k % 2
        for q in range(2):
            pltpu.matmul_push_rhs(w, staging_register=reg, mxu_index=q)
        for n in range(len(accs[0])):
            for q in range(2):
                a = lhs_piece(one, o + q, row_of(n))
                b = lhs_piece(two, o + q, row_of(n)) if two is not None else a
                pltpu.matmul_acc_lhs(
                    accs[q][n], jnp.concatenate([a, b], axis=1), load_staged_rhs=reg if n == 0 else None
                )

    n_main = (len(main_chunks) + 1) // 2
    n_pair = len(pair_chunks) // 2

    def pop_main(accs, q, r):
        pm[q, r] = pltpu.matmul_pop(accs[q][r])

    def pop_pair(accs, q, n):
        v = pltpu.matmul_pop(accs[q][n])
        p3[q, 2 * n] = v[:, :LANE]
        p3[q, 2 * n + 1] = v[:, LANE:]

    def share(todo, k, lead, span):
        k -= lead
        if k < 0 or k >= span:
            return []
        return todo[k * len(todo) // span : (k + 1) * len(todo) // span]

    def out_copy(i):
        here = pl.ds(2 * i, 2)
        there = here if not final else pl.ds(x_start + 2 * i, 2)
        return pltpu.make_async_copy(o_buf.at[here], outs[0].at[there], o_sem.at[i])

    def body(main_accs, pair_accs):
        for q in range(2):
            for acc in main_accs[q] + pair_accs[q]:
                pltpu.matmul_pop(acc)

        def first_frames(f, carry):
            for rs in range(half + 2):
                put(build(f, rs))
            return carry

        lax.fori_loop(0, min(4, n_in), first_frames, 0)
        for c in w_copies:
            c.wait()
        if final:
            x_copy.wait()

        def step(i, carry):
            o = 2 * i
            done = jnp.maximum(o - 2, 0)
            live = i > 0
            todo = [(q, r, j) for q in range(2) for r, j in units]
            lead = 3
            pending = []
            for k in range(n_main):
                run_pass(main_chunks, k, main_weight, main_accs, o, lambda n: n)
                if k == 1:
                    for q in range(2):
                        for n in range(half // 2):
                            pop_pair(pair_accs, q, n)
                put(pending)
                pending = []
                for q, r, j in share(todo, k, lead, n_main - lead - 2):
                    if r == half:
                        put(pending)
                        pending = []
                    pending += finish(q, done + q, r, j, live)
            put(pending)

            new = jnp.minimum(o + 4, n_in - 2)
            todo = [(q, rs) for q in range(2) for rs in range(half + 2)]
            lead = 10
            pending = []
            for k in range(n_pair):
                run_pass(pair_chunks, k, pair_weight, pair_accs, o, lambda n: 2 * n)
                if 4 <= k < 4 + half // 2:
                    for q in range(2):
                        for r in range(2 * (k - 4), 2 * (k - 4) + 2):
                            pop_main(main_accs, q, r)
                put(pending)
                pending = []
                for q, rs in share(todo, k, lead, n_pair - lead - 2):
                    pending += build(new + q, rs)
            put(pending)

            @pl.when(i > 0)
            def _():
                out_copy(i - 1).start()

            return carry

        lax.fori_loop(0, steps, step, 0)
        for q in range(2):
            for n in range(half // 2):
                pop_pair(pair_accs, q, n)
        for q in range(2):
            for r, j in units:
                put(finish(q, n_out - 2 + q, r, j))
        last = [out_copy(steps - 1)]
        if not final:
            for e in range(2):
                last.append(pltpu.make_async_copy(row_buf.at[e], outs[1 + e], b_sem.at[e]))
                last.append(pltpu.make_async_copy(col_buf.at[e], outs[3 + e], b_sem.at[2 + e]))
            last.append(pltpu.make_async_copy(o_buf.at[pl.ds(n_out - 2, 2)], outs[5], b_sem.at[4]))
        for c in last:
            c.start()
        for i in range(steps - 1):
            out_copy(i).wait()
        for c in last:
            c.wait()

    pl.run_scoped(
        body,
        tuple(tuple(pltpu.ACC(q)((wide, 2 * LANE), F32) for _ in range(half)) for q in range(2)),
        tuple(tuple(pltpu.ACC(q)((wide, 2 * LANE), F32) for _ in range(half // 2)) for q in range(2)),
    )


def conv(segments, flags, parity, weights, bias, gain, layer, rows, width, x=None, x_start=0, into=None):
    blocks = -(-width // SUB)
    cols = blocks * SUB
    chans = weights.shape[-1]
    operands, cfg_segs = [], []
    corner_rows = 0
    for kind, arrays, start, count in segments:
        which = []
        for a in arrays:
            known = [n for n, b in enumerate(operands) if b is a]
            if not known:
                operands.append(a)
            which.append(known[0] if known else len(operands) - 1)
        cfg_segs.append((kind, tuple(which), start, count))
        corner_rows += arrays[1].shape[0] - arrays[0].shape[0] if kind == "own" else count
    n_ops = len(operands)
    n_in = sum(count for _, _, _, count in segments)
    n_out = n_in - 2
    half = rows // 2
    wide = blocks * 16
    final = 0 if x is None else (1 if into is None else 2)
    cfg = (tuple(cfg_segs), n_ops, n_in, rows, blocks, chans, layer, (width - 1) % SUB, final, x_start)
    any_spec = pl.BlockSpec(memory_space=pltpu.HBM)
    vmem_spec = pl.BlockSpec(memory_space=pltpu.VMEM)
    operands += [flags, parity, weights, bias, gain]
    in_specs = [any_spec] * n_ops + [pl.BlockSpec(memory_space=pltpu.SMEM)] * 2 + [any_spec, vmem_spec, vmem_spec]
    aliases = {}
    if final:
        operands.append(x)
        in_specs.append(any_spec)
        if final == 2:
            aliases = {len(operands): 0}
            operands.append(into)
            in_specs.append(any_spec)
        out_shape = [jax.ShapeDtypeStruct(x.shape, F32)]
        o_buf = pltpu.VMEM((n_out, rows, cols, chans), F32)
    else:
        out_shape = [
            jax.ShapeDtypeStruct((n_out, n, chans), BF16) for n in (rows * cols, cols, cols, rows, rows)
        ]
        out_shape.append(jax.ShapeDtypeStruct((2, rows * cols, chans), BF16))
        o_buf = pltpu.VMEM((n_out, rows * cols, chans), BF16)
    n_border = 1 if final else n_out
    copies = sum(7 if kind == "own" else 6 for kind, _, _, count in segments)
    scratch = [
        ((chans // LANE, 3, n_in, half + 2, wide, LANE), BF16),
        ((chans // LANE, 3, 3, 3, chans, LANE), BF16),
        ((n_in, rows * cols, chans), BF16),
        ((2, n_in, cols, chans), BF16),
        ((2, n_in, rows, chans), BF16),
        ((2, corner_rows, cols, chans), BF16),
        ((2, n_in, cols, chans), F32),
        ((2, n_in, rows, chans), F32),
        ((2, 2 * n_in, chans), F32),
        ((2, half, wide, 2 * LANE), F32),
        ((2, half, wide, LANE), F32),
        (o_buf.shape, o_buf.dtype),
        ((2, 2, cols, chans), F32),
        ((2, 2, rows, chans), F32),
        ((2, n_border, cols, chans), BF16),
        ((2, n_border, rows, chans), BF16),
    ]
    cells = n_out * rows * cols
    out = pl.pallas_call(
        lambda *refs: conv_kernel(cfg, *refs),
        out_shape=out_shape,
        in_specs=in_specs,
        out_specs=[any_spec] * len(out_shape),
        scratch_shapes=[pltpu.VMEM(shape, dtype) for shape, dtype in scratch]
        + [
            pltpu.SemaphoreType.DMA((copies,)),
            pltpu.SemaphoreType.DMA((3, chans // LANE)),
            pltpu.SemaphoreType.DMA,
            pltpu.SemaphoreType.DMA((n_out // 2,)),
            pltpu.SemaphoreType.DMA((5,)),
        ],
        input_output_aliases=aliases,
        compiler_params=pltpu.CompilerParams(vmem_limit_bytes=60 << 20),
        cost_estimate=pl.CostEstimate(
            flops=2 * 27 * cells * chans * chans, bytes_accessed=8 * cells * chans, transcendentals=0
        ),
        name="conv_final" if final else "conv_first",
    )(*operands)
    return out[0] if final else out


def along(x, axis, by):
    size = lax.axis_size(axis)
    return lax.ppermute(x, axis, [(i, i + by) for i in range(size) if 0 <= i + by < size])


def side_flags():
    at, size = lax.axis_index("col"), lax.axis_size("col")
    return jnp.stack([at > 0, at < size - 1]).astype(F32)


def row_parity():
    return (1 - lax.axis_index("row") % 2).astype(jnp.int32)


def row_swaps(below, above):
    size = lax.axis_size("row")
    even = row_parity() == 1
    got = []
    for start, mine in ((0, jnp.where(even, below, above)), (1, jnp.where(even, above, below))):
        pairs = [(i, i + 1) for i in range(start, size - 1, 2)]
        got.append(lax.ppermute(mine, "row", pairs + [(b, a) for a, b in pairs]))
    return got


def exchange(first_row, last_row, first_col, last_col):
    n, cols, chans = first_row.shape
    if lax.axis_size("col") == 2:
        mine = jnp.where(lax.axis_index("col") == 0, last_col, first_col)
        left = right = lax.ppermute(mine, "col", [(0, 1), (1, 0)])
    else:
        left = along(last_col, "col", 1)
        right = along(first_col, "col", -1)
    extra = -(-2 * n // cols)

    def payload(row, at):
        corners = jnp.stack([left[:, at], right[:, at]], axis=1).reshape(2 * n, chans)
        corners = jnp.pad(corners, ((0, extra * cols - 2 * n), (0, 0)))
        return jnp.concatenate([row, corners.reshape(extra, cols, chans)], axis=0)

    below, above = payload(last_row, -1), payload(first_row, 0)
    return *row_swaps(below, above), left, right


def from_earlier(tail, halo):
    top, bottom, left, right = halo
    n, _, chans = left.shape
    parts = [top[n - 2 : n], bottom[n - 2 : n], left[-2:], right[-2:]]
    for part in (top, bottom):
        parts.append(part[n:].reshape(-1, chans)[2 * n - 4 : 2 * n].reshape(2, 2, chans))
    parts.append(jnp.zeros((2, SUB - 4, chans), BF16))
    return along(tail, "ta", 1), along(jnp.concatenate(parts, axis=1), "ta", 1)


def shards(latent_in, norm_gains, conv_weights, conv_bias):
    frames, rows, width, chans = latent_in.shape
    pad = -width % SUB
    x = jnp.pad(latent_in, ((0, 0), (0, 0), (0, pad), (0, 0))) if pad else latent_in
    flags = side_flags()
    late = frames // 2
    last = frames // 4

    tiles, *border, tail = prepare(x, norm_gains[0:1], width)
    halo = exchange(*border)
    early = from_earlier(tail, halo)
    first = dict(flags=flags, parity=row_parity()[None], weights=conv_weights, bias=conv_bias[0:1], gain=norm_gains[1:2],
                 layer=0, rows=rows, width=width)
    second = dict(first, bias=conv_bias[1:2], layer=1, x=x)

    own = (tiles, *halo)
    tiles_b, *border_b, tail = conv([("own", own, late - 2, frames - late + 2)], **first)
    own_b = (tiles_b, *exchange(*border_b))
    tiles_a, *border_a, _ = conv([("rec", early, 0, 2), ("own", own, 0, late)], **first)
    early = from_earlier(tail, own_b[1:])
    own_a = (tiles_a, *exchange(*border_a))
    cut = frames - late - last
    out = conv([("own", own_b, cut - 2, last + 2)], **second, x_start=frames - last)
    out = conv(
        [("rec", early, 0, 2), ("own", own_a, 0, late), ("own", own_b, 0, cut)],
        **second, x_start=0, into=out,
    )
    return out[:, :, :width] if pad else out


def solution(mesh):
    placed = (P("ta", "row", "col", None), P(), P(), P())
    return jax.shard_map(
        shards, mesh=mesh, in_specs=placed, out_specs=P("ta", "row", "col", None), check_vma=False
    )
```

```python
import jax
import jax.numpy as jnp
from jax import lax
from jax.experimental import pallas as pl
from jax.experimental.pallas import tpu as pltpu
from jax.sharding import PartitionSpec as P

EPS = 1e-06
SUB = 8
LANE = 128
F32 = jnp.float32
BF16 = jnp.bfloat16


def activate(value, gain):
    mean_sq = jnp.mean(value * value, axis=-1, keepdims=True)
    u = value * lax.rsqrt(mean_sq + EPS) * gain
    return (u / (1.0 + jnp.exp(-u))).astype(BF16)


def border_parts(value, r, j, half, blocks, last_valid):
    parts = []
    if r == 0:
        parts.append(("row", 0, j * SUB, value[0:SUB]))
    if r == half - 1:
        parts.append(("row", 1, j * SUB, value[SUB:16]))
    if j == 0:
        parts.append(("col", 0, r, value[0:1]))
        parts.append(("col", 0, r + half, value[SUB : SUB + 1]))
    if j == blocks - 1:
        parts.append(("col", 1, r, value[last_valid : last_valid + 1]))
        parts.append(("col", 1, r + half, value[SUB + last_valid : SUB + last_valid + 1]))
    return parts


def prepare_kernel(last_valid, total, x_ref, gain_ref, pick_ref, out_ref, row0, row1, col0, col1, tail_ref, row_f, col_f):
    half, blocks = x_ref.shape[1] // 2, x_ref.shape[2] // SUB
    count = x_ref.shape[0]
    gain = gain_ref[...]
    even, side = pick_ref[0], pick_ref[1]

    def frame(k, carry):
        kept = jnp.maximum(pl.program_id(0) * count + k - (total - 2), 0)
        for r in range(half):
            for j in range(blocks):
                cols = pl.ds(j * SUB, SUB)
                v = jnp.concatenate([x_ref[k, r, cols, :], x_ref[k, r + half, cols, :]], axis=0)
                a = activate(v, gain)
                here = pl.ds((r * blocks + j) * 16, 16)
                out_ref[k, here, :] = a
                tail_ref[kept, here, :] = a
                for kind, e, row, piece in border_parts(a.astype(F32), r, j, half, blocks, last_valid):
                    dst = row_f if kind == "row" else col_f
                    dst[e, pl.ds(row, piece.shape[0]), :] = piece
        row0[k] = row_f[even].astype(BF16)
        row1[k] = row_f[1 - even].astype(BF16)
        col0[k] = col_f[side].astype(BF16)
        col1[k] = col_f[1 - side].astype(BF16)
        return carry

    lax.fori_loop(0, count, frame, 0)


def extra_frames(n, cols):
    return -(-2 * n // cols)


def record_rows(rows, cols):
    return rows * cols + 2 * (rows + cols) + SUB


def prepare(x, gain, picks, width):
    frames, rows, cols, chans = x.shape
    cells = rows * cols
    step = 4 if frames % 4 == 0 else 1
    m = extra_frames(frames, cols)

    def spec(n):
        return pl.BlockSpec((step, n, chans), lambda f: (f, 0, 0))

    sizes = ((cells, 0), (cols, m), (cols, m), (rows, 0), (rows, 0))
    keep = (2, record_rows(rows, cols), chans)
    return pl.pallas_call(
        lambda *refs: prepare_kernel((width - 1) % SUB, frames, *refs),
        out_shape=[jax.ShapeDtypeStruct((frames + more, n, chans), BF16) for n, more in sizes]
        + [jax.ShapeDtypeStruct(keep, BF16)],
        grid=(frames // step,),
        in_specs=[
            pl.BlockSpec((step, rows, cols, chans), lambda f: (f, 0, 0, 0)),
            pl.BlockSpec((1, chans), lambda f: (0, 0)),
            pl.BlockSpec(memory_space=pltpu.SMEM),
        ],
        out_specs=[spec(n) for n, _ in sizes] + [pl.BlockSpec(keep, lambda f: (0, 0, 0))],
        scratch_shapes=[pltpu.VMEM((2, cols, chans), F32), pltpu.VMEM((2, rows, chans), F32)],
        compiler_params=pltpu.CompilerParams(vmem_limit_bytes=60 << 20),
        cost_estimate=pl.CostEstimate(flops=20 * x.size, bytes_accessed=6 * x.size, transcendentals=2 * x.size),
        name="prepare",
    )(x, gain, picks)


def conv_kernel(cfg, *refs):
    segs, n_ops, n_in, rows, blocks, chans, layer, last_valid, final, x_start = cfg
    n_out = n_in - 2
    steps = n_out // 2
    half = rows // 2
    cols = blocks * SUB
    wide = blocks * 16
    n_chunk = chans // LANE
    ins = refs[:n_ops]
    at = n_ops
    flag_ref, pick_ref, w_hbm, bias_ref, gain_ref = refs[at : at + 5]
    at += 5
    if final:
        x_hbm = refs[at]
        at += 2 if final == 2 else 1
        outs = refs[at : at + 1]
        at += 1
    else:
        outs = refs[at : at + 6]
        at += 6
    (a_buf, w_buf, t_buf, edge_buf, side_buf, corner_buf, edge_f, side_f, corner_f, pm, p3, o_buf,
     row_f, col_f, row_buf, col_buf, in_sem, w_sem, x_sem, o_sem, b_sem) = refs[at:]
    taps = [(dt, dr, dc) for dt in range(3) for dr in range(3) for dc in range(3)]
    even, side = pick_ref[0], pick_ref[1]
    slots = (even, 1 - even)

    copies = []

    def fetch(src, dst):
        copies.append(pltpu.make_async_copy(src, dst, in_sem.at[len(copies)]))

    base = 0
    corner_at = 0
    corners = []
    earlier = []
    for kind, which, start, count in segs:
        here = pl.ds(base, count)
        if kind == "own":
            t, top, bot, lft, rgt = [ins[n] for n in which]
            there = pl.ds(start, count)
            fetch(t.at[there], t_buf.at[here])
            frames = t.shape[0]
            extra = top.shape[0] - frames
            for e, part in ((0, top), (1, bot)):
                fetch(part.at[there], edge_buf.at[e, here])
                fetch(part.at[pl.ds(frames, extra)], corner_buf.at[e, pl.ds(corner_at, extra)])
                corners.append((e, e, corner_at, extra, 2 * start, base, count))
            for e, part in ((0, lft), (1, rgt)):
                fetch(part.at[there], side_buf.at[e, here])
            corner_at += extra
        else:
            (rec,) = [ins[n] for n in which]
            off = rows * cols
            fetch(rec.at[:, pl.ds(0, off)], t_buf.at[here])
            for e in range(2):
                fetch(rec.at[:, pl.ds(off + e * cols, cols)], edge_buf.at[e, here])
                fetch(rec.at[:, pl.ds(off + 2 * cols + e * rows, rows)], side_buf.at[e, here])
            off += 2 * (cols + rows)
            fetch(rec.at[:, pl.ds(off, SUB)], corner_buf.at[0, pl.ds(corner_at, count), pl.ds(0, SUB)])
            earlier.append((here, pl.ds(corner_at, count)))
            for e in range(2):
                for k in range(count):
                    corners.append((e, 0, corner_at + k, 1, 2 * e, base + k, 1))
            corner_at += count
        base += count
    w_copies = [
        pltpu.make_async_copy(
            w_hbm.at[layer, dt, :, :, :, pl.ds(oc * LANE, LANE)], w_buf.at[oc, dt], w_sem.at[dt, oc]
        )
        for dt in range(3)
        for oc in range(n_chunk)
    ]
    for c in copies:
        c.start()
    for c in copies:
        c.wait()
    for c in w_copies:
        c.start()

    for here, corner_here in earlier:

        @pl.when(pick_ref[2] == 0)
        def _():
            t_buf[here] = jnp.zeros((2, rows * cols, chans), BF16)
            for e in range(2):
                edge_buf[e, here] = jnp.zeros((2, cols, chans), BF16)
                side_buf[e, here] = jnp.zeros((2, rows, chans), BF16)
            corner_buf[0, corner_here] = jnp.zeros((2, cols, chans), BF16)

    def widen(f, carry):
        for e in range(2):
            edge_f[e, f] = edge_buf[e, f].astype(F32) * flag_ref[2 + e]
            side_f[e, f] = side_buf[e, f].astype(F32) * flag_ref[e]
        return carry

    lax.fori_loop(0, n_in, widen, 0)
    for e, source, where, extra, first, base_, count in corners:
        block = corner_buf[source, pl.ds(where, extra)].astype(F32).reshape(extra * cols, chans)
        corner_f[e, pl.ds(2 * base_, 2 * count), :] = block[first : first + 2 * count] * flag_ref[2 + e]

    sub_index = lax.broadcasted_iota(jnp.int32, (SUB, chans), 0)
    is_first = sub_index == 0
    is_last = sub_index == SUB - 1
    is_valid_last = sub_index == last_valid

    def tile_at(f, r, j):
        return t_buf[f, pl.ds((r * blocks + j) * 16, 16), :]

    def beside(e, f, row):
        if row < 0 or row >= rows:
            value = corner_f[slots[0 if row < 0 else 1], pl.ds(2 * f + e, 1), :] * flag_ref[e]
        else:
            value = side_f[e, f, pl.ds(row, 1), :]
        return jnp.broadcast_to(value, (SUB, chans))

    def build(f, rs):
        tiles = []
        for j in range(blocks):
            if 1 <= rs <= half:
                tiles.append(tile_at(f, rs - 1, j))
            elif rs == 0:
                upper = edge_f[slots[0], f, pl.ds(j * SUB, SUB), :]
                lower = tile_at(f, half - 1, j).astype(F32)[0:SUB]
                tiles.append(jnp.concatenate([upper, lower], axis=0).astype(BF16))
            else:
                upper = tile_at(f, 0, j).astype(F32)[SUB:16]
                lower = edge_f[slots[1], f, pl.ds(j * SUB, SUB), :]
                tiles.append(jnp.concatenate([upper, lower], axis=0).astype(BF16))
        shifted = [[[None, None] for _ in range(blocks)] for _ in range(2)]
        for h in range(2):
            row = rs - 1 + half * h
            left = beside(0, f, row)
            right = beside(1, f, row)
            parts = [t.astype(F32)[h * SUB : (h + 1) * SUB] for t in tiles]
            down = [left] + [pltpu.roll(p, 1, 0) for p in parts]
            up = [pltpu.roll(p, SUB - 1, 0) for p in parts]
            for j in range(blocks):
                shifted[0][j][h] = jnp.where(is_first, down[j], down[j + 1])
                if j + 1 < blocks:
                    shifted[1][j][h] = jnp.where(is_last, up[j + 1], up[j])
                else:
                    shifted[1][j][h] = jnp.where(is_valid_last, right, up[j])
        stores = []
        for j in range(blocks):
            low = jnp.concatenate(shifted[0][j], axis=0).astype(BF16)
            high = jnp.concatenate(shifted[1][j], axis=0).astype(BF16)
            for dc, value in ((0, low), (1, tiles[j]), (2, high)):
                for kc in range(n_chunk):
                    part = value[:, kc * LANE : (kc + 1) * LANE]
                    stores.append((a_buf, (kc, dc, f, rs, pl.ds(j * 16, 16), slice(None)), part))
        return stores

    def put(stores):
        for ref, index, value in stores:
            ref[index] = value

    def finish(q, f, r, j):
        if r == half:
            stores = []
            for e in range(2):
                stores.append((row_buf, (e, f), row_f[q, e].astype(BF16)))
                stores.append((col_buf, (e, f), col_f[q, e].astype(BF16)))
            return stores
        sl = pl.ds(j * 16, 16)
        v = jnp.concatenate([pm[q, r, sl, :], p3[q, r, sl, :]], axis=1) + bias_ref[...]
        if not final:
            a = activate(v, gain_ref[...])
            stores = [(o_buf, (f, pl.ds((r * blocks + j) * 16, 16), slice(None)), a)]
            for kind, e, row, piece in border_parts(a.astype(F32), r, j, half, blocks, last_valid):
                dst = row_f if kind == "row" else col_f
                stores.append((dst, (q, e, pl.ds(row, piece.shape[0]), slice(None)), piece))
            return stores
        stores = []
        for h in range(2):
            index = (f, r + half * h, pl.ds(j * SUB, SUB), slice(None))
            part = v[h * SUB : (h + 1) * SUB]
            stores.append((o_buf, index, o_buf[index] + part))
        return stores

    units = [(r, j) for r in range(half) for j in range(blocks)]
    if not final:
        units.append((half, 0))

    main_chunks = [(tap, kc) for tap in taps for kc in range(n_chunk)]
    pair_chunks = [
        ((dt, drp, dc), kc)
        for dt in range(3) for drp in range(4) for dc in range(3) for kc in range(n_chunk)
    ]

    def main_weight(chunk):
        if chunk is None:
            return jnp.zeros((LANE, 2 * LANE), BF16)
        (dt, dr, dc), kc = chunk
        here = pl.ds(kc * LANE, LANE)
        return jnp.concatenate([w_buf[0, dt, dr, dc, here, :], w_buf[1, dt, dr, dc, here, :]], axis=1)

    def pair_weight(chunk):
        (dt, drp, dc), kc = chunk
        sides = []
        for dr in (drp, drp - 1):
            if 0 <= dr <= 2:
                sides.append(w_buf[2, dt, dr, dc, pl.ds(kc * LANE, LANE), :])
            else:
                sides.append(jnp.zeros((LANE, LANE), BF16))
        return jnp.concatenate(sides, axis=1)

    def lhs_piece(chunk, o, r):
        (dt, dr, dc), kc = chunk
        return a_buf[kc, dc, o + dt, r + dr]

    def run_pass(chunks, k, weight, accs, o, row_of):
        one = chunks[2 * k]
        two = chunks[2 * k + 1] if 2 * k + 1 < len(chunks) else None
        w = jnp.concatenate([weight(one), weight(two)], axis=0)
        reg = k % 2
        for q in range(2):
            pltpu.matmul_push_rhs(w, staging_register=reg, mxu_index=q)
        for n in range(len(accs[0])):
            for q in range(2):
                a = lhs_piece(one, o + q, row_of(n))
                b = lhs_piece(two, o + q, row_of(n)) if two is not None else a
                pltpu.matmul_acc_lhs(
                    accs[q][n], jnp.concatenate([a, b], axis=1), load_staged_rhs=reg if n == 0 else None
                )

    n_main = (len(main_chunks) + 1) // 2
    n_pair = len(pair_chunks) // 2

    def pop_main(accs, q, r):
        pm[q, r] = pltpu.matmul_pop(accs[q][r])

    def pop_pair(accs, q, n):
        v = pltpu.matmul_pop(accs[q][n])
        p3[q, 2 * n] = v[:, :LANE]
        p3[q, 2 * n + 1] = v[:, LANE:]

    def share(todo, k, lead, span):
        k -= lead
        if k < 0 or k >= span:
            return []
        return todo[k * len(todo) // span : (k + 1) * len(todo) // span]

    def out_copy(i):
        here = pl.ds(2 * i, 2)
        there = here if not final else pl.ds(x_start + 2 * i, 2)
        return pltpu.make_async_copy(o_buf.at[here], outs[0].at[there], o_sem.at[i])

    def body(main_accs, pair_accs):
        for q in range(2):
            for acc in main_accs[q] + pair_accs[q]:
                pltpu.matmul_pop(acc)

        def first_frames(f, carry):
            for rs in range(half + 2):
                put(build(f, rs))
            return carry

        lax.fori_loop(0, min(4, n_in), first_frames, 0)
        for c in w_copies:
            c.wait()
        if final:
            x_copy = pltpu.make_async_copy(x_hbm.at[pl.ds(x_start, n_out)], o_buf.at[pl.ds(0, n_out)], x_sem)
            x_copy.start()
            if steps == 1:
                x_copy.wait()

        def step(i, carry):
            o = 2 * i
            if final:
                done = jnp.where(i > 0, o - 2, n_out)

                @pl.when(i == 1)
                def _():
                    x_copy.wait()
            else:
                done = jnp.maximum(o - 2, 0)
            todo = [(q, r, j) for q in range(2) for r, j in units]
            lead = 3
            pending = []
            for k in range(n_main):
                run_pass(main_chunks, k, main_weight, main_accs, o, lambda n: n)
                if k == 1:
                    for q in range(2):
                        for n in range(half // 2):
                            pop_pair(pair_accs, q, n)
                put(pending)
                pending = []
                for q, r, j in share(todo, k, lead, n_main - lead - 2):
                    if r == half:
                        put(pending)
                        pending = []
                    pending += finish(q, done + q, r, j)
            put(pending)

            new = jnp.minimum(o + 4, n_in - 2)
            todo = [(q, rs) for q in range(2) for rs in range(half + 2)]
            lead = 10
            pending = []
            for k in range(n_pair):
                run_pass(pair_chunks, k, pair_weight, pair_accs, o, lambda n: 2 * n)
                if 4 <= k < 4 + half // 2:
                    for q in range(2):
                        for r in range(2 * (k - 4), 2 * (k - 4) + 2):
                            pop_main(main_accs, q, r)
                put(pending)
                pending = []
                for q, rs in share(todo, k, lead, n_pair - lead - 2):
                    pending += build(new + q, rs)
            put(pending)

            @pl.when(i > 0)
            def _():
                out_copy(i - 1).start()

            return carry

        lax.fori_loop(0, steps, step, 0)
        for q in range(2):
            for n in range(half // 2):
                pop_pair(pair_accs, q, n)
        for q in range(2):
            for r, j in units:
                put(finish(q, n_out - 2 + q, r, j))
        last = [out_copy(steps - 1)]
        if not final:
            for e in range(2):
                row_from = even if e == 0 else 1 - even
                col_from = side if e == 0 else 1 - side
                row_to = outs[1 + e].at[pl.ds(0, n_out)]
                last.append(pltpu.make_async_copy(row_buf.at[row_from], row_to, b_sem.at[e]))
                last.append(pltpu.make_async_copy(col_buf.at[col_from], outs[3 + e], b_sem.at[2 + e]))
            tail_to = outs[5].at[:, pl.ds(0, rows * cols)]
            last.append(pltpu.make_async_copy(o_buf.at[pl.ds(n_out - 2, 2)], tail_to, b_sem.at[4]))
        for c in last:
            c.start()
        for i in range(steps - 1):
            out_copy(i).wait()
        for c in last:
            c.wait()

    pl.run_scoped(
        body,
        tuple(tuple(pltpu.ACC(q)((wide, 2 * LANE), F32) for _ in range(half)) for q in range(2)),
        tuple(tuple(pltpu.ACC(q)((wide, 2 * LANE), F32) for _ in range(half // 2)) for q in range(2)),
    )


def conv(segments, flags, picks, weights, bias, gain, layer, rows, width, x=None, x_start=0, into=None):
    blocks = -(-width // SUB)
    cols = blocks * SUB
    chans = weights.shape[-1]
    operands, cfg_segs = [], []
    corner_rows = 0
    for kind, arrays, start, count in segments:
        which = []
        for a in arrays:
            known = [n for n, b in enumerate(operands) if b is a]
            if not known:
                operands.append(a)
            which.append(known[0] if known else len(operands) - 1)
        cfg_segs.append((kind, tuple(which), start, count))
        corner_rows += arrays[1].shape[0] - arrays[0].shape[0] if kind == "own" else count
    n_ops = len(operands)
    n_in = sum(count for _, _, _, count in segments)
    n_out = n_in - 2
    half = rows // 2
    wide = blocks * 16
    m = extra_frames(n_out, cols)
    final = 0 if x is None else (1 if into is None else 2)
    cfg = (tuple(cfg_segs), n_ops, n_in, rows, blocks, chans, layer, (width - 1) % SUB, final, x_start)
    any_spec = pl.BlockSpec(memory_space=pltpu.HBM)
    vmem_spec = pl.BlockSpec(memory_space=pltpu.VMEM)
    operands += [flags, picks, weights, bias, gain]
    in_specs = [any_spec] * n_ops + [pl.BlockSpec(memory_space=pltpu.SMEM)] * 2 + [any_spec, vmem_spec, vmem_spec]
    aliases = {}
    if final:
        operands.append(x)
        in_specs.append(any_spec)
        if final == 2:
            aliases = {len(operands): 0}
            operands.append(into)
            in_specs.append(any_spec)
        out_shape = [jax.ShapeDtypeStruct(x.shape, F32)]
        o_buf = pltpu.VMEM((n_out + 2, rows, cols, chans), F32)
    else:
        out_shape = [
            jax.ShapeDtypeStruct((n_out + more, n, chans), BF16)
            for n, more in ((rows * cols, 0), (cols, m), (cols, m), (rows, 0), (rows, 0))
        ]
        out_shape.append(jax.ShapeDtypeStruct((2, record_rows(rows, cols), chans), BF16))
        o_buf = pltpu.VMEM((n_out, rows * cols, chans), BF16)
    n_border = 1 if final else n_out
    copies = sum(7 if kind == "own" else 6 for kind, _, _, count in segments)
    scratch = [
        ((chans // LANE, 3, n_in, half + 2, wide, LANE), BF16),
        ((chans // LANE, 3, 3, 3, chans, LANE), BF16),
        ((n_in, rows * cols, chans), BF16),
        ((2, n_in, cols, chans), BF16),
        ((2, n_in, rows, chans), BF16),
        ((2, corner_rows, cols, chans), BF16),
        ((2, n_in, cols, chans), F32),
        ((2, n_in, rows, chans), F32),
        ((2, 2 * n_in, chans), F32),
        ((2, half, wide, 2 * LANE), F32),
        ((2, half, wide, LANE), F32),
        (o_buf.shape, o_buf.dtype),
        ((2, 2, cols, chans), F32),
        ((2, 2, rows, chans), F32),
        ((2, n_border, cols, chans), BF16),
        ((2, n_border, rows, chans), BF16),
    ]
    cells = n_out * rows * cols
    out = pl.pallas_call(
        lambda *refs: conv_kernel(cfg, *refs),
        out_shape=out_shape,
        in_specs=in_specs,
        out_specs=[any_spec] * len(out_shape),
        scratch_shapes=[pltpu.VMEM(shape, dtype) for shape, dtype in scratch]
        + [
            pltpu.SemaphoreType.DMA((copies,)),
            pltpu.SemaphoreType.DMA((3, chans // LANE)),
            pltpu.SemaphoreType.DMA,
            pltpu.SemaphoreType.DMA((n_out // 2,)),
            pltpu.SemaphoreType.DMA((5,)),
        ],
        input_output_aliases=aliases,
        compiler_params=pltpu.CompilerParams(vmem_limit_bytes=60 << 20),
        cost_estimate=pl.CostEstimate(
            flops=2 * 27 * cells * chans * chans, bytes_accessed=8 * cells * chans, transcendentals=0
        ),
        name="conv_final" if final else "conv_first",
    )(*operands)
    return out[0] if final else out


def along(x, axis, by):
    size = lax.axis_size(axis)
    return lax.ppermute(x, axis, [(i, i + by) for i in range(size) if 0 <= i + by < size])


def neighbours():
    row, col = lax.axis_index("row"), lax.axis_index("col")
    rows, cols = lax.axis_size("row"), lax.axis_size("col")
    even = 1 - row % 2
    second = jnp.where(even == 1, row > 0, row < rows - 1)
    flags = jnp.stack([col > 0, col < cols - 1, jnp.bool_(True), second]).astype(F32)
    side = 1 - col if cols == 2 else jnp.zeros_like(col)
    picks = jnp.stack([even, side, lax.axis_index("ta")]).astype(jnp.int32)
    return flags, picks


def row_swaps(first, second):
    size = lax.axis_size("row")
    got = []
    for start, mine in ((0, first), (1, second)):
        pairs = [(i, i + 1) for i in range(start, size - 1, 2)]
        got.append(lax.ppermute(mine, "row", pairs + [(b, a) for a, b in pairs]))
    return got


def exchange(even, row_a, row_b, col_a, col_b):
    n, _, chans = col_a.shape
    cols = row_a.shape[1]
    if lax.axis_size("col") == 2:
        left = right = lax.ppermute(col_a, "col", [(0, 1), (1, 0)])
    else:
        left = along(col_b, "col", 1)
        right = along(col_a, "col", -1)
    extra = extra_frames(n, cols)

    def payload(row, last):
        corners = [jnp.where(last, side[:, -1], side[:, 0]) for side in (left, right)]
        corners = jnp.stack(corners, axis=1).reshape(2 * n, chans)
        corners = jnp.pad(corners, ((0, extra * cols - 2 * n), (0, 0)))
        return lax.dynamic_update_slice(row, corners.reshape(extra, cols, chans), (n, 0, 0))

    rows = payload(row_a, even == 1), payload(row_b, even == 0)
    return *row_swaps(*rows), left, right


def from_earlier(record, halo):
    a, b, left, right = halo
    n, _, chans = left.shape
    parts = [a[n - 2 : n], b[n - 2 : n], left[-2:], right[-2:]]
    for part in (a, b):
        parts.append(part[n:].reshape(-1, chans)[2 * n - 4 : 2 * n].reshape(2, 2, chans))
    parts.append(jnp.zeros((2, SUB - 4, chans), BF16))
    packed = jnp.concatenate(parts, axis=1)
    record = lax.dynamic_update_slice(record, packed, (0, record.shape[1] - packed.shape[1], 0))
    size = lax.axis_size("ta")
    return lax.ppermute(record, "ta", [(i, (i + 1) % size) for i in range(size)])


def shards(latent_in, norm_gains, conv_weights, conv_bias):
    frames, rows, width, chans = latent_in.shape
    pad = -width % SUB
    x = jnp.pad(latent_in, ((0, 0), (0, 0), (0, pad), (0, 0))) if pad else latent_in
    flags, picks = neighbours()
    late = frames // 2
    last = frames // 4

    tiles, *border, tail = prepare(x, norm_gains[0:1], picks, width)
    halo = exchange(picks[0], *border)
    early = from_earlier(tail, halo)
    first = dict(flags=flags, picks=picks, weights=conv_weights, bias=conv_bias[0:1], gain=norm_gains[1:2],
                 layer=0, rows=rows, width=width)
    second = dict(first, bias=conv_bias[1:2], layer=1, x=x)

    own = (tiles, *halo)
    tiles_b, *border_b, tail = conv([("own", own, late - 2, frames - late + 2)], **first)
    own_b = (tiles_b, *exchange(picks[0], *border_b))
    tiles_a, *border_a, _ = conv([("rec", (early,), 0, 2), ("own", own, 0, late)], **first)
    early = from_earlier(tail, own_b[1:])
    own_a = (tiles_a, *exchange(picks[0], *border_a))
    cut = frames - late - last
    out = conv([("own", own_b, cut - 2, last + 2)], **second, x_start=frames - last)
    out = conv(
        [("rec", (early,), 0, 2), ("own", own_a, 0, late), ("own", own_b, 0, cut)],
        **second, x_start=0, into=out,
    )
    return out[:, :, :width] if pad else out


def solution(mesh):
    placed = (P("ta", "row", "col", None), P(), P(), P())
    return jax.shard_map(
        shards, mesh=mesh, in_specs=placed, out_specs=P("ta", "row", "col", None), check_vma=False
    )
```
